32 devices in a mesh: dp: 4 (over z), vocab: 8 (over y, x, core).
Axes of the slice: x: 2, y: 2, z: 4, core: 2. Of those that a mesh axis runs over, the one named last changes fastest.
Arguments:
- hidden: bfloat16 [512, 4096], P(('dp', 'vocab')), may hold values from -64 to 64
- head_weight: bfloat16 [4096, 128256], P(None, ('dp', 'vocab')), may hold values from -0.0625 to 0.0625
- targets: int32 [512], P(('dp', 'vocab')), may hold values from 0 to 128255
- bench_ids: int32 [512], P(('dp', 'vocab')), may hold values from 0 to 39, as said below
- valid: int32 [512], P(('dp', 'vocab')), may hold values from 0 to 1, as said below
- seq_lengths: int32 [16], replicated, may hold values from 1 to 64, 512 in all
Outputs:
- token_loss: float32 [512], P(('dp', 'vocab'))
- bench_loss: float32 [40], replicated
- bench_count: float32 [40], replicated
The draws below stay inside these ranges and needn't reach their ends.
Inputs may be any that keep to these rules, and one draw needn't show every extreme that they name: `valid`: among the 16 positions of one device (aligned blocks) at most 8 have validity 1, and some block has exactly 8. `bench_ids`: A benchmark may have no positions in the window.
All inputs are finite; a program needn't handle non-finite values.
Results may differ from the reference program's by a relative error of at most 0.0003.
Values may be sent and summed in bfloat16 or wider, within the bound.
A program may use at most 128 MiB of HBM per device.

```python
import math
import jax
import jax.numpy as jnp
import numpy as np
from jax import lax

D = 4096
VOCAB = 128256
BENCH = 40
TOK_DEV = 16
TOKENS = 512
SEQS = 16
MAXLEN = 64


def head_column(key, column_id):
    column_key = jax.random.fold_in(jax.random.fold_in(key, 4242), column_id)
    values = jnp.clip(jax.random.normal(column_key, (D,), jnp.float32), -4.0, 4.0) * D ** (-0.5)
    return values.astype(jnp.bfloat16).astype(jnp.float32)


def draw_head_weight(key, part):
    columns = jax.vmap(head_column, in_axes=(None, 0))(key, jnp.arange(VOCAB, dtype=jnp.int32))
    return columns.T.astype(jnp.bfloat16)


def draw_hidden(key, part):
    normal_part = jax.random.normal(jax.random.fold_in(key, 17), (TOKENS, D), jnp.float32)
    values = 3.0 * jnp.clip(normal_part, -5.0, 5.0)
    return values.astype(jnp.bfloat16)


def draw_bench_ids(key, part):
    order = jax.random.permutation(jax.random.fold_in(key, 51), BENCH).astype(jnp.int32)
    first_rank = jax.random.randint(jax.random.fold_in(key, 52), (TOKENS,), 0, BENCH - 1)
    second_rank = jax.random.randint(jax.random.fold_in(key, 53), (TOKENS,), 0, BENCH - 1)
    ranks = jnp.minimum(first_rank, second_rank)
    return order[ranks].astype(jnp.int32)


def permuted(key_item):
    return jax.random.permutation(key_item, TOK_DEV)


def draw_valid(key, part):
    device_count = TOKENS // TOK_DEV
    capacity = TOK_DEV // 2
    fewest = max(capacity // 3, 1)
    per_device = jax.random.randint(jax.random.fold_in(key, 31), (device_count,), fewest, capacity + 1)
    busiest = jax.random.randint(jax.random.fold_in(key, 32), (), 0, device_count)
    bottom = (busiest + 1 + jax.random.randint(jax.random.fold_in(key, 33), (), 0, device_count - 1)) % device_count
    per_device = per_device.at[busiest].set(capacity).at[bottom].set(fewest)
    rank_table = jax.vmap(permuted)(jax.random.split(jax.random.fold_in(key, 34), device_count))
    return (rank_table < per_device[:, None]).astype(jnp.int32).reshape(TOKENS)


def plant(drawn, own_key, least, high):
    dims = drawn.shape
    index_at = [jax.random.randint(jax.random.fold_in(own_key, axis), (), 0, dims[axis]) for axis in range(len(dims))]
    drawn = drawn.at[tuple(index_at)].set(least)
    longest = dims.index(max(dims))
    index_at[longest] = (index_at[longest] + 1) % dims[longest]
    return drawn.at[tuple(index_at)].set(high)


def wide_ids(own_key, dims, amount, skew):
    weights = [min(1 << octave, amount + 1 - (1 << octave)) * (1 << 20) // math.isqrt((1 << octave) ** skew) + 1 for octave in range((amount + 1).bit_length()) if 1 << octave <= amount]
    scale = 1 + sum(weights) // (1 << 30)
    listing = np.cumsum(np.array([max(1, weight // scale) for weight in weights]))
    ticket = jax.random.randint(jax.random.fold_in(own_key, 1), dims, 0, int(listing[len(weights) - 1]))
    start = jnp.left_shift(1, jnp.searchsorted(jnp.asarray(listing, jnp.int32), ticket, side="right").astype(jnp.int32))
    rank = start - 1 + jax.random.randint(jax.random.fold_in(own_key, 4), dims, 0, 1 << 30) % jnp.minimum(start, amount + 1 - start)
    return jax.random.permutation(jax.random.fold_in(own_key, 2), amount)[rank].astype(jnp.int32)


def length_profile(count, total, limit, skew):
    portions = [(1 << 20) // math.isqrt(standing ** skew) + 1 for standing in range(2, count + 1)]
    rest, counts = total - limit - (count - 1), [1] * (count - 1)
    while rest > 0:
        candidates = [i for i in range(count - 1) if counts[i] < limit]
        whole, left = sum([portions[i] for i in candidates]), rest
        for i in candidates:
            addition = min(limit - counts[i], max(1, left * portions[i] // whole), rest)
            counts[i] = counts[i] + addition
            rest = rest - addition
    return np.array([limit] + counts)


def ragged(key, amount, total, bound, lean):
    if amount == 2:
        one = jax.random.randint(key, (), max(1, total - bound), min(bound, total - 1) + 1)
        return jnp.stack([one, total - one])
    sizes = jnp.asarray(length_profile(amount, total, bound, lean), jnp.int32)
    pairs = (amount - 1) // 2
    source_of, sink = sizes[1:1 + 2 * pairs:2], sizes[2:2 + 2 * pairs:2]
    slack = jnp.minimum(source_of - 1, bound - sink)
    passed = jax.random.randint(jax.random.fold_in(key, 1), (pairs,), 0, 1 << 20) % (slack + 1)
    sizes = sizes.at[1:1 + 2 * pairs:2].set(source_of - passed).at[2:2 + 2 * pairs:2].set(sink + passed)
    return sizes[jax.random.permutation(jax.random.fold_in(key, 2), amount)]


def setup_inputs(seed: int = 0) -> dict:
    streams_of = jax.random.split(jax.random.key(seed), 7)
    return {
        "hidden": draw_hidden(jax.random.fold_in(streams_of[6], 71), 0),
        "head_weight": draw_head_weight(jax.random.fold_in(streams_of[6], 71), 0),
        "targets": plant(wide_ids(streams_of[2], (TOKENS,), VOCAB, 2), jax.random.fold_in(streams_of[2], 3), 0, VOCAB - 1).astype(jnp.int32),
        "bench_ids": draw_bench_ids(jax.random.fold_in(streams_of[6], 71), 0),
        "valid": draw_valid(jax.random.fold_in(streams_of[6], 71), 0),
        "seq_lengths": ragged(streams_of[5], SEQS, TOKENS, MAXLEN, 2).astype(jnp.int32),
    }


def reference(hidden, head_weight, targets, bench_ids, valid, seq_lengths):
    seq_ends = (jnp.cumsum(seq_lengths) - 1).astype(jnp.int32)
    positions = jnp.arange(TOKENS, dtype=jnp.int32)
    is_end = jnp.any(positions[:, None] == seq_ends[None, :], axis=1)
    scored = valid * (1 - is_end.astype(jnp.int32))

    def score_block(inputs):
        row_block, target_ids = inputs
        logits = jnp.dot(row_block, head_weight, preferred_element_type=jnp.float32)
        row_top = jnp.max(logits, axis=1)
        row_total = jnp.sum(jnp.exp(logits - row_top[:, None]), axis=1)
        target_logit = jnp.take_along_axis(logits, target_ids[:, None], axis=1)[:, 0]
        return row_top + jnp.log(row_total) - target_logit

    losses = lax.map(score_block, (hidden.reshape(TOKENS // TOK_DEV, TOK_DEV, D), targets.reshape(TOKENS // TOK_DEV, TOK_DEV)))
    scored_float = scored.astype(jnp.float32)
    token_loss = losses.reshape(TOKENS) * scored_float
    onehot = (bench_ids[:, None] == jnp.arange(BENCH, dtype=jnp.int32)[None, :]).astype(jnp.float32)
    loss_sums = jnp.sum(onehot * token_loss[:, None], axis=0)
    token_counts = jnp.sum(onehot * scored_float[:, None], axis=0)
    bench_loss = loss_sums / jnp.maximum(token_counts, 1.0)
    return (token_loss, bench_loss, token_counts)
```

```python
import functools

import jax
import jax.numpy as jnp
from jax import lax
from jax.experimental import pallas as pl
from jax.experimental.pallas import tpu as pltpu
from jax.sharding import PartitionSpec as P

BENCH = 40
AXES = ("dp", "vocab")
PARTS = 4
MESH = pl.DeviceIdType.MESH


def toggled(index, mask):
    return index + mask - 2 * mask * ((index // mask) % 2)


def runs_of(done):
    slots = [0]
    for bit in done:
        slots = slots + [slot + (1 << bit) for slot in slots]
    slots.sort()
    runs = []
    for slot in slots:
        if runs and runs[-1][0] + runs[-1][1] == slot:
            runs[-1][1] += 1
        else:
            runs.append([slot, 1])
    return runs


def kernel(
    n, vocab_size, hidden, weight, targets, bench_ids, valid, lengths,
    token_loss, bench_loss, bench_count,
    x_own, x_far, w_own, w_far, acc, labels, mine_own, mine_far, mine_lab,
    their_own, their_far, their_lab, stats, packed, gathered,
    w_sems, pair_send, pair_recv, hop_send, hop_recv, fwd_send, fwd_recv, st_send, st_recv,
):
    rows, depth = hidden.shape
    cols = weight.shape[1]
    kp = depth // (2 * PARTS)
    chips = n // 2
    bits = chips.bit_length() - 1
    total = chips * rows
    half = rows // 2
    me = lax.axis_index("dp") * vocab_size + lax.axis_index("vocab")
    core = me % 2
    chip = me // 2
    chip_bits = [(i + bits // 2) % bits for i in range(bits)]
    slot_me = sum(((chip // (1 << chip_bits[b])) % 2) * (1 << b) for b in range(bits))

    def place(index):
        return (index // vocab_size, index % vocab_size)

    partner = place(toggled(me, 1))

    def w_copy(far, j):
        which = (1 - core) if far else core
        start = pl.multiple_of((which * PARTS + j) * kp, kp)
        dst = (w_far if far else w_own).at[j]
        return pltpu.make_async_copy(weight.at[pl.ds(start, kp), :], dst, w_sems.at[int(far), j])

    order = []
    for j in range(PARTS):
        order.append((False, j))
        if j:
            order.append((True, j - 1))
    order.append((True, PARTS - 1))
    for far, j in order:
        w_copy(far, j).start()

    barrier = pltpu.get_barrier_semaphore()

    @pl.loop(1, n)
    def _(d):
        pl.semaphore_signal(barrier, inc=1, device_id=place((me + d) % n), device_id_type=MESH)

    lane = lax.broadcasted_iota(jnp.int32, (rows, rows), 1)
    sub = lax.broadcasted_iota(jnp.int32, (rows, rows), 0)
    eye = lane == sub

    def to_col(row):
        return jnp.sum(jnp.where(eye, jnp.broadcast_to(row, (rows, rows)), 0.0), axis=1, keepdims=True)

    pos = me * rows + lax.broadcasted_iota(jnp.int32, (1, rows), 1)
    live = valid[...]
    run = jnp.int32(0)
    for j in range(lengths.shape[0]):
        run = run + lengths[j]
        live = jnp.where(pos == run - 1, 0, live)
    live_row = live.astype(jnp.float32)
    live_col = to_col(live_row)
    tgt_col = to_col(targets[...].astype(jnp.float32))
    ben_col = to_col(bench_ids[...].astype(jnp.float32))
    rank_row = jnp.sum(jnp.where(sub <= lane, live_col, 0.0), axis=0, keepdims=True)
    rank_col = to_col(rank_row)
    spot_row = rank_row - 1.0 + (core * half).astype(jnp.float32)
    pick = jnp.where(sub.astype(jnp.float32) == spot_row, live_row, 0.0)
    pick_bf = pick.astype(jnp.bfloat16)
    lab_lane = lax.broadcasted_iota(jnp.int32, (rows, 128), 1)
    lab_in = jnp.where(lab_lane == 0, tgt_col, 0.0)
    lab_in = jnp.where(lab_lane == 1, ben_col, lab_in)
    lab_in = jnp.where(lab_lane == 2, live_col, lab_in)
    lab = jnp.zeros((rows, 128), jnp.float32)
    for j in range(rows):
        lab = lab + pick[:, j:j + 1] * lab_in[j:j + 1, :]
    mine_lab[...] = lab
    for j in range(PARTS):
        for far, dst in ((False, mine_own), (True, mine_far)):
            which = (1 - core) if far else core
            start = pl.multiple_of((which * PARTS + j) * kp, kp)
            dst[j] = jnp.dot(
                pick_bf, hidden[:, pl.ds(start, kp)], preferred_element_type=jnp.float32
            ).astype(jnp.bfloat16)

    pl.semaphore_wait(barrier, n - 1)

    pair = []
    for i, (src, dst) in enumerate(((mine_lab, their_lab), (mine_far, their_own), (mine_own, their_far))):
        copy = pltpu.make_async_remote_copy(
            src_ref=src, dst_ref=dst, send_sem=pair_send.at[i], recv_sem=pair_recv.at[i],
            device_id=partner, device_id_type=MESH)
        copy.start()
        pair.append(copy)
    pair[0].wait_recv()
    labels[0:rows, :] = mine_lab[...] + their_lab[...]
    pair[1].wait_recv()
    for j in range(PARTS):
        x_own[j, 0:rows, :] = mine_own[j] + their_own[j]

    count = [0]
    sends = []

    def hop(ref, bit, done):
        target = place(toggled(me, 2 << chip_bits[bit]))
        copies = []
        for start, length in runs_of(done):
            src = ref.at[pl.ds(start * rows, length * rows), :]
            dst = ref.at[pl.ds((start + (1 << bit)) * rows, length * rows), :]
            i = count[0]
            count[0] += 1
            copy = pltpu.make_async_remote_copy(
                src_ref=src, dst_ref=dst, send_sem=hop_send.at[i], recv_sem=hop_recv.at[i],
                device_id=target, device_id_type=MESH)
            copy.start()
            copies.append(copy)
        sends.extend(copies)
        return copies

    plan_a = list(range(bits))
    plan_b = plan_a[:-2] + [plan_a[-1], plan_a[-2]] if bits >= 2 else plan_a
    streams = [(labels, plan_a)] + [(x_own.at[j], plan_b if j % 2 else plan_a) for j in range(PARTS)]
    flying = [[] for _ in streams]
    for step in range(bits):
        for i, (ref, plan) in enumerate(streams):
            for copy in flying[i]:
                copy.wait_recv()
            flying[i] = hop(ref, plan[step], plan[:step])
        if step == 0:
            pair[2].wait_recv()
            for j in range(PARTS):
                x_far[j, 0:rows, :] = mine_far[j] + their_far[j]
    for copy in flying[0]:
        copy.wait_recv()

    def forward(j):
        return pltpu.make_async_remote_copy(
            src_ref=x_own.at[j, pl.ds(rows, total - rows), :],
            dst_ref=x_far.at[j, pl.ds(rows, total - rows), :],
            send_sem=fwd_send.at[j], recv_sem=fwd_recv.at[j],
            device_id=partner, device_id_type=MESH)

    width = 1024

    def multiply(far, j, first):
        w_copy(far, j).wait()
        x = (x_far if far else x_own)[j]
        w = (w_far if far else w_own).at[j]
        for start in range(0, cols, width):
            stop = min(cols, start + width)
            part = jnp.dot(x, w[:, start:stop], preferred_element_type=jnp.float32)
            if first:
                acc[:, start:stop] = part
            else:
                acc[:, start:stop] += part

    for far, j in order:
        if far:
            forward(j).wait_recv()
        else:
            for copy in flying[j + 1]:
                copy.wait_recv()
            forward(j).start()
        multiply(far, j, first=(not far and j == 0))

    block = 64
    offset = me * cols

    @pl.loop(0, total // block)
    def _(i):
        start = pl.multiple_of(i * block, block)
        lab = labels[pl.ds(start, block), :]
        ids = lab[:, 0:1].astype(jnp.int32) - offset
        values = acc[pl.ds(start, block), :]
        column = lax.broadcasted_iota(jnp.int32, (block, cols), 1)
        goal = jnp.sum(jnp.where(column == ids, values, 0.0), axis=1, keepdims=True)
        top = jnp.max(values, axis=1, keepdims=True)
        summed = jnp.sum(jnp.exp(values - top), axis=1, keepdims=True)
        at = lax.broadcasted_iota(jnp.int32, (block, 128), 1)
        out = jnp.where(at == 0, top, 0.0)
        out = jnp.where(at == 1, summed, out)
        out = jnp.where(at == 2, goal, out)
        out = jnp.where(at == 3, lab[:, 1:2], out)
        out = jnp.where(at == 4, lab[:, 2:3], out)
        for k in range(block // rows):
            slot = i * (block // rows) + k
            true_slot = sum(
                (((slot // (1 << b)) % 2 + (slot_me // (1 << b)) % 2) % 2) * (1 << b) for b in range(bits))
            stats[pl.ds(pl.multiple_of(true_slot * rows, rows), rows), :] = out[k * rows:(k + 1) * rows]

    lanes = [stats[b * 128:(b + 1) * 128, :].T for b in range(total // 128)]
    packed[...] = jnp.concatenate([t[0:4, :] for t in lanes], axis=0)
    ben_lane = [t[3:4, :] for t in lanes]
    live_lane = [t[4:5, :] for t in lanes]

    def st_copy(d):
        return pltpu.make_async_remote_copy(
            src_ref=packed, dst_ref=gathered.at[me], send_sem=st_send.at[d], recv_sem=st_recv.at[me],
            device_id=place((me + d) % n), device_id_type=MESH)

    @pl.loop(1, n)
    def _(d):
        st_copy(d).start()

    gathered[me] = packed[...]
    for copy in pair + sends + [forward(j) for j in range(PARTS)]:
        copy.wait_send()

    @pl.loop(1, n)
    def _(d):
        st_copy(d).wait_send()
        source = (me + d) % n
        pltpu.make_async_remote_copy(
            src_ref=packed, dst_ref=gathered.at[source], send_sem=st_send.at[d],
            recv_sem=st_recv.at[source], device_id=place(source), device_id_type=MESH).wait_recv()

    bench = lax.broadcasted_iota(jnp.int32, (BENCH, 128), 0).astype(jnp.float32)
    sums = jnp.zeros((BENCH, 1), jnp.float32)
    counts = jnp.zeros((BENCH, 1), jnp.float32)
    own = jnp.zeros((rows, 1), jnp.float32)
    spot = (slot_me * rows + core * half).astype(jnp.float32) + rank_col - 1.0
    for b in range(total // 128):
        tops = gathered[:, 4 * b, :]
        best = jnp.max(tops, axis=0, keepdims=True)
        summed = jnp.sum(gathered[:, 4 * b + 1, :] * jnp.exp(tops - best), axis=0, keepdims=True)
        goal = jnp.sum(gathered[:, 4 * b + 2, :], axis=0, keepdims=True)
        loss = best + jnp.log(summed) - goal
        hot = jnp.where(bench == ben_lane[b], live_lane[b], 0.0)
        sums = sums + jnp.sum(hot * loss, axis=1, keepdims=True)
        counts = counts + jnp.sum(hot, axis=1, keepdims=True)
        where = (lax.broadcasted_iota(jnp.int32, (rows, 128), 1) + b * 128).astype(jnp.float32)
        own = own + jnp.sum(jnp.where(where == spot, loss, 0.0), axis=1, keepdims=True)

    def to_row(col):
        size = col.shape[0]
        square = lax.broadcasted_iota(jnp.int32, (size, size), 0) == lax.broadcasted_iota(jnp.int32, (size, size), 1)
        return jnp.sum(jnp.where(square, col, 0.0), axis=0, keepdims=True)

    token_loss[...] = to_row(own * live_col)
    bench_loss[...] = to_row(sums / jnp.maximum(counts, 1.0))
    bench_count[...] = to_row(counts)


def body(hidden, head_weight, targets, bench_ids, valid, seq_lengths):
    n = lax.axis_size(AXES)
    vocab_size = lax.axis_size("vocab")
    rows, depth = hidden.shape
    cols = head_weight.shape[1]
    chips = n // 2
    bits = chips.bit_length() - 1
    total = chips * rows
    kp = depth // (2 * PARTS)
    hops = bits + PARTS * (bits + 1)
    bf, f32 = jnp.bfloat16, jnp.float32
    vmem = pl.BlockSpec(memory_space=pltpu.VMEM)
    dma = pltpu.SemaphoreType.DMA
    out = pl.pallas_call(
        functools.partial(kernel, n, vocab_size),
        out_shape=(
            jax.ShapeDtypeStruct((1, rows), f32),
            jax.ShapeDtypeStruct((1, BENCH), f32),
            jax.ShapeDtypeStruct((1, BENCH), f32),
        ),
        in_specs=[vmem, pl.BlockSpec(memory_space=pl.ANY), vmem, vmem, vmem,
                  pl.BlockSpec(memory_space=pltpu.SMEM)],
        out_specs=(vmem, vmem, vmem),
        scratch_shapes=[
            pltpu.VMEM((PARTS, total, kp), bf),
            pltpu.VMEM((PARTS, total, kp), bf),
            pltpu.VMEM((PARTS, kp, cols), bf),
            pltpu.VMEM((PARTS, kp, cols), bf),
            pltpu.VMEM((total, cols), f32),
            pltpu.VMEM((total, 128), f32),
            pltpu.VMEM((PARTS, rows, kp), bf),
            pltpu.VMEM((PARTS, rows, kp), bf),
            pltpu.VMEM((rows, 128), f32),
            pltpu.VMEM((PARTS, rows, kp), bf),
            pltpu.VMEM((PARTS, rows, kp), bf),
            pltpu.VMEM((rows, 128), f32),
            pltpu.VMEM((total, 128), f32),
            pltpu.VMEM((total // 32, 128), f32),
            pltpu.VMEM((n, total // 32, 128), f32),
            dma((2, PARTS)), dma((3,)), dma((3,)), dma((hops,)), dma((hops,)),
            dma((PARTS,)), dma((PARTS,)), dma((n,)), dma((n,)),
        ],
        compiler_params=pltpu.CompilerParams(
            collective_id=0, has_side_effects=True, vmem_limit_bytes=60 << 20),
    )(hidden, head_weight, targets.reshape(1, rows), bench_ids.reshape(1, rows),
      valid.reshape(1, rows), seq_lengths)
    return out[0].reshape(rows), out[1].reshape(BENCH), out[2].reshape(BENCH)


def solution(mesh):
    placed = (
        P(AXES, None),
        P(None, AXES),
        P(AXES),
        P(AXES),
        P(AXES),
        P(),
    )
    return jax.shard_map(
        body, mesh=mesh, in_specs=placed, out_specs=(P(AXES), P(), P()), check_vma=False
    )
```

```python
import functools

import jax
import jax.numpy as jnp
from jax import lax
from jax.experimental import pallas as pl
from jax.experimental.pallas import tpu as pltpu
from jax.sharding import PartitionSpec as P

BENCH = 40
AXES = ("dp", "vocab")
PARTS = 4
MESH = pl.DeviceIdType.MESH


def toggled(index, mask):
    return index + mask - 2 * mask * ((index // mask) % 2)


def runs_of(done):
    slots = [0]
    for bit in done:
        slots = slots + [slot + (1 << bit) for slot in slots]
    slots.sort()
    runs = []
    for slot in slots:
        if runs and runs[-1][0] + runs[-1][1] == slot:
            runs[-1][1] += 1
        else:
            runs.append([slot, 1])
    return runs


def kernel(
    n, vocab_size, hidden, weight, targets, bench_ids, valid, lengths,
    result,
    x_own, x_far, w_own, w_far, acc, labels, mine_own, mine_far, mine_lab,
    their_own, their_far, their_lab, stats, packed, gathered,
    w_sems, pair_send, pair_recv, hop_send, hop_recv, fwd_send, fwd_recv, st_send, st_recv,
):
    rows, depth = hidden.shape
    cols = weight.shape[0]
    kp = depth // (2 * PARTS)
    chips = n // 2
    bits = chips.bit_length() - 1
    total = chips * rows
    half = rows // 2
    me = lax.axis_index("dp") * vocab_size + lax.axis_index("vocab")
    core = me % 2
    chip = me // 2
    chip_bits = [(i + bits // 2) % bits for i in range(bits)]
    slot_me = sum(((chip // (1 << chip_bits[b])) % 2) * (1 << b) for b in range(bits))

    def place(index):
        return (index // vocab_size, index % vocab_size)

    partner = place(toggled(me, 1))

    def w_copy(far, j):
        which = (1 - core) if far else core
        start = pl.multiple_of((which * PARTS + j) * kp, kp)
        dst = (w_far if far else w_own).at[j]
        return pltpu.make_async_copy(weight.at[:, pl.ds(start, kp)], dst, w_sems.at[int(far), j])

    order = []
    for j in range(PARTS):
        order.append((False, j))
        if j:
            order.append((True, j - 1))
    order.append((True, PARTS - 1))
    for far, j in order:
        w_copy(far, j).start()

    barrier = pltpu.get_barrier_semaphore()

    @pl.loop(1, n)
    def _(d):
        pl.semaphore_signal(barrier, inc=1, device_id=place((me + d) % n), device_id_type=MESH)

    lane = lax.broadcasted_iota(jnp.int32, (rows, rows), 1)
    sub = lax.broadcasted_iota(jnp.int32, (rows, rows), 0)
    eye = lane == sub

    def to_col(row):
        return jnp.sum(jnp.where(eye, jnp.broadcast_to(row, (rows, rows)), 0.0), axis=1, keepdims=True)

    pos = me * rows + lax.broadcasted_iota(jnp.int32, (1, rows), 1)
    live = valid[...]
    run = jnp.int32(0)
    for j in range(lengths.shape[0]):
        run = run + lengths[j]
        live = jnp.where(pos == run - 1, 0, live)
    live_row = live.astype(jnp.float32)
    live_col = to_col(live_row)
    tgt_col = to_col(targets[...].astype(jnp.float32))
    ben_col = to_col(bench_ids[...].astype(jnp.float32))
    rank_row = jnp.sum(jnp.where(sub <= lane, live_col, 0.0), axis=0, keepdims=True)
    rank_col = to_col(rank_row)
    spot_row = rank_row - 1.0 + (core * half).astype(jnp.float32)
    pick = jnp.where(sub.astype(jnp.float32) == spot_row, live_row, 0.0)
    pick_bf = pick.astype(jnp.bfloat16)
    lab_lane = lax.broadcasted_iota(jnp.int32, (rows, 128), 1)
    lab_in = jnp.where(lab_lane == 0, tgt_col, 0.0)
    lab_in = jnp.where(lab_lane == 1, ben_col, lab_in)
    lab_in = jnp.where(lab_lane == 2, live_col, lab_in)
    lab = jnp.zeros((rows, 128), jnp.float32)
    for j in range(rows):
        lab = lab + pick[:, j:j + 1] * lab_in[j:j + 1, :]
    mine_lab[...] = lab
    for j in range(PARTS):
        for far, dst in ((False, mine_own), (True, mine_far)):
            which = (1 - core) if far else core
            start = pl.multiple_of((which * PARTS + j) * kp, kp)
            dst[j] = jnp.dot(
                pick_bf, hidden[:, pl.ds(start, kp)], preferred_element_type=jnp.float32
            ).astype(jnp.bfloat16)

    pl.semaphore_wait(barrier, n - 1)

    pair = []
    for i, (src, dst) in enumerate(((mine_lab, their_lab), (mine_far, their_own), (mine_own, their_far))):
        copy = pltpu.make_async_remote_copy(
            src_ref=src, dst_ref=dst, send_sem=pair_send.at[i], recv_sem=pair_recv.at[i],
            device_id=partner, device_id_type=MESH)
        copy.start()
        pair.append(copy)
    pair[0].wait_recv()
    labels[0:rows, :] = mine_lab[...] + their_lab[...]
    pair[1].wait_recv()
    for j in range(PARTS):
        x_own[j, 0:rows, :] = mine_own[j] + their_own[j]

    count = [0]
    sends = []

    def hop(ref, bit, done):
        target = place(toggled(me, 2 << chip_bits[bit]))
        copies = []
        for start, length in runs_of(done):
            src = ref.at[pl.ds(start * rows, length * rows), :]
            dst = ref.at[pl.ds((start + (1 << bit)) * rows, length * rows), :]
            i = count[0]
            count[0] += 1
            copy = pltpu.make_async_remote_copy(
                src_ref=src, dst_ref=dst, send_sem=hop_send.at[i], recv_sem=hop_recv.at[i],
                device_id=target, device_id_type=MESH)
            copy.start()
            copies.append(copy)
        sends.extend(copies)
        return copies

    plan_a = list(range(bits))
    plan_b = plan_a[:-2] + [plan_a[-1], plan_a[-2]] if bits >= 2 else plan_a
    streams = [(labels, plan_a)] + [(x_own.at[j], plan_b if j % 2 else plan_a) for j in range(PARTS)]
    flying = [[] for _ in streams]
    for step in range(bits):
        for i, (ref, plan) in enumerate(streams):
            for copy in flying[i]:
                copy.wait_recv()
            flying[i] = hop(ref, plan[step], plan[:step])
        if step == 0:
            pair[2].wait_recv()
            for j in range(PARTS):
                x_far[j, 0:rows, :] = mine_far[j] + their_far[j]
    for copy in flying[0]:
        copy.wait_recv()

    def forward(j):
        return pltpu.make_async_remote_copy(
            src_ref=x_own.at[j, pl.ds(rows, total - rows), :],
            dst_ref=x_far.at[j, pl.ds(rows, total - rows), :],
            send_sem=fwd_send.at[j], recv_sem=fwd_recv.at[j],
            device_id=partner, device_id_type=MESH)

    width = 1024

    def multiply(far, j, first):
        w_copy(far, j).wait()
        x = (x_far if far else x_own)[j]
        w = (w_far if far else w_own).at[j]
        for start in range(0, cols, width):
            stop = min(cols, start + width)
            part = lax.dot_general(
                w[start:stop, :], x, (((1,), (1,)), ((), ())), preferred_element_type=jnp.float32)
            if first:
                acc[start:stop, :] = part
            else:
                acc[start:stop, :] += part

    for far, j in order:
        if far:
            forward(j).wait_recv()
        else:
            for copy in flying[j + 1]:
                copy.wait_recv()
            forward(j).start()
        multiply(far, j, first=(not far and j == 0))

    offset = me * cols
    label_lanes = [labels[b * 128:(b + 1) * 128, :].T for b in range(total // 128)]
    ids = jnp.concatenate([t[0:1, :] for t in label_lanes], axis=1).astype(jnp.int32) - offset
    block = 128
    full = cols // block
    tail = cols - full * block

    def fold(values, op):
        size = values.shape[0]
        whole = size // 8 * 8
        out = op(values[:whole].reshape(whole // 8, 8, total), axis=0)
        return op(out, axis=0, keepdims=True), values[whole:]

    def scan(op, merge, init, make):
        def reduced(values):
            out, rest = fold(values, op)
            return merge(out, op(rest, axis=0, keepdims=True)) if rest.shape[0] else out

        def wide(i, carry):
            values = make(pl.multiple_of(i * block, block), block)
            return merge(carry, op(values.reshape(block // 8, 8, total), axis=0))

        carry = lax.fori_loop(0, full, wide, jnp.full((8, total), init, jnp.float32))
        out = op(carry, axis=0, keepdims=True)
        if tail:
            out = merge(out, reduced(make(full * block, tail)))
        return out

    def load(start, size):
        return acc[pl.ds(start, size), :]

    top = scan(jnp.max, jnp.maximum, -jnp.inf, load)
    summed = scan(jnp.sum, jnp.add, 0.0, lambda start, size: jnp.exp(load(start, size) - top))

    def hits(start, size):
        row = lax.broadcasted_iota(jnp.int32, (size, total), 0) + start
        return jnp.where(row == ids, load(start, size), 0.0)

    goal = scan(jnp.sum, jnp.add, 0.0, hits)
    at = lax.broadcasted_iota(jnp.int32, (128, 128), 1)
    for b in range(total // 128):
        part = slice(b * 128, (b + 1) * 128)
        rest = jnp.zeros((125, 128), jnp.float32)
        cols_of = jnp.concatenate([top[:, part], summed[:, part], goal[:, part], rest], axis=0).T
        lab = labels[part, :]
        out = jnp.where(at == 3, lab[:, 1:2], cols_of)
        out = jnp.where(at == 4, lab[:, 2:3], out)
        for k in range(128 // rows):
            slot = b * (128 // rows) + k
            true_slot = sum(
                (((slot // (1 << c)) % 2 + (slot_me // (1 << c)) % 2) % 2) * (1 << c) for c in range(bits))
            stats[pl.ds(pl.multiple_of(true_slot * rows, rows), rows), :] = out[k * rows:(k + 1) * rows]

    lanes = [stats[b * 128:(b + 1) * 128, :].T for b in range(total // 128)]
    packed[...] = jnp.concatenate([t[0:4, :] for t in lanes], axis=0)
    ben_lane = [t[3:4, :] for t in lanes]
    live_lane = [t[4:5, :] for t in lanes]

    def st_copy(d):
        return pltpu.make_async_remote_copy(
            src_ref=packed, dst_ref=gathered.at[me], send_sem=st_send.at[d], recv_sem=st_recv.at[me],
            device_id=place((me + d) % n), device_id_type=MESH)

    @pl.loop(1, n)
    def _(d):
        st_copy(d).start()

    gathered[me] = packed[...]
    for copy in pair + sends + [forward(j) for j in range(PARTS)]:
        copy.wait_send()

    @pl.loop(1, n)
    def _(d):
        st_copy(d).wait_send()
        source = (me + d) % n
        pltpu.make_async_remote_copy(
            src_ref=packed, dst_ref=gathered.at[source], send_sem=st_send.at[d],
            recv_sem=st_recv.at[source], device_id=place(source), device_id_type=MESH).wait_recv()

    bench = lax.broadcasted_iota(jnp.int32, (BENCH, 128), 0).astype(jnp.float32)
    sums = jnp.zeros((BENCH, 1), jnp.float32)
    counts = jnp.zeros((BENCH, 1), jnp.float32)
    own = jnp.zeros((rows, 1), jnp.float32)
    spot = (slot_me * rows + core * half).astype(jnp.float32) + rank_col - 1.0
    for b in range(total // 128):
        tops = gathered[:, 4 * b, :]
        best = jnp.max(tops, axis=0, keepdims=True)
        summed = jnp.sum(gathered[:, 4 * b + 1, :] * jnp.exp(tops - best), axis=0, keepdims=True)
        goal = jnp.sum(gathered[:, 4 * b + 2, :], axis=0, keepdims=True)
        loss = best + jnp.log(summed) - goal
        hot = jnp.where(bench == ben_lane[b], live_lane[b], 0.0)
        sums = sums + jnp.sum(hot * loss, axis=1, keepdims=True)
        counts = counts + jnp.sum(hot, axis=1, keepdims=True)
        where = (lax.broadcasted_iota(jnp.int32, (rows, 128), 1) + b * 128).astype(jnp.float32)
        own = own + jnp.sum(jnp.where(where == spot, loss, 0.0), axis=1, keepdims=True)

    def to_row(col):
        size = col.shape[0]
        square = lax.broadcasted_iota(jnp.int32, (size, size), 0) == lax.broadcasted_iota(jnp.int32, (size, size), 1)
        return jnp.sum(jnp.where(square, col, 0.0), axis=0, keepdims=True)

    result[...] = jnp.zeros(result.shape, jnp.float32)
    result[0:1, 0:rows] = to_row(own * live_col)
    result[1:2, 0:BENCH] = to_row(sums)
    result[2:3, 0:BENCH] = to_row(counts)


def body(hidden, head_weight, targets, bench_ids, valid, seq_lengths):
    n = lax.axis_size(AXES)
    vocab_size = lax.axis_size("vocab")
    rows, depth = hidden.shape
    cols = head_weight.shape[1]
    chips = n // 2
    bits = chips.bit_length() - 1
    total = chips * rows
    kp = depth // (2 * PARTS)
    hops = bits + PARTS * (bits + 1)
    bf, f32 = jnp.bfloat16, jnp.float32
    vmem = pl.BlockSpec(memory_space=pltpu.VMEM)
    dma = pltpu.SemaphoreType.DMA
    out = pl.pallas_call(
        functools.partial(kernel, n, vocab_size),
        out_shape=jax.ShapeDtypeStruct((8, 128), f32),
        in_specs=[vmem, pl.BlockSpec(memory_space=pl.ANY), vmem, vmem, vmem,
                  pl.BlockSpec(memory_space=pltpu.SMEM)],
        out_specs=vmem,
        scratch_shapes=[
            pltpu.VMEM((PARTS, total, kp), bf),
            pltpu.VMEM((PARTS, total, kp), bf),
            pltpu.VMEM((PARTS, cols, kp), bf),
            pltpu.VMEM((PARTS, cols, kp), bf),
            pltpu.VMEM((cols, total), f32),
            pltpu.VMEM((total, 128), f32),
            pltpu.VMEM((PARTS, rows, kp), bf),
            pltpu.VMEM((PARTS, rows, kp), bf),
            pltpu.VMEM((rows, 128), f32),
            pltpu.VMEM((PARTS, rows, kp), bf),
            pltpu.VMEM((PARTS, rows, kp), bf),
            pltpu.VMEM((rows, 128), f32),
            pltpu.VMEM((total, 128), f32),
            pltpu.VMEM((total // 32, 128), f32),
            pltpu.VMEM((n, total // 32, 128), f32),
            dma((2, PARTS)), dma((3,)), dma((3,)), dma((hops,)), dma((hops,)),
            dma((PARTS,)), dma((PARTS,)), dma((n,)), dma((n,)),
        ],
        compiler_params=pltpu.CompilerParams(
            collective_id=0, has_side_effects=True, vmem_limit_bytes=60 << 20),
    )(hidden, head_weight.T, targets.reshape(1, rows), bench_ids.reshape(1, rows),
      valid.reshape(1, rows), seq_lengths)
    counts = out[2, :BENCH]
    return out[0, :rows], out[1, :BENCH] / jnp.maximum(counts, 1.0), counts


def solution(mesh):
    placed = (
        P(AXES, None),
        P(None, AXES),
        P(AXES),
        P(AXES),
        P(AXES),
        P(),
    )
    return jax.shard_map(
        body, mesh=mesh, in_specs=placed, out_specs=(P(AXES), P(), P()), check_vma=False
    )
```
